32 devices in a mesh: batch: 8 (over z, x), head: 4 (over y, core).
Axes of the slice: x: 2, y: 2, z: 4, core: 2. Of those that a mesh axis runs over, the one named last changes fastest.
Arguments:
- tokens: bfloat16 [4096, 2048], P('batch', 'head'), may hold values from -96 to 96
- lengths: int32 [32], P('batch'), may hold values from 1 to 128
- states: float32 [32, 16, 128, 128], P('batch', 'head'), may hold values from -3 to 3
- norm_gain: float32 [2048], replicated, may hold values from 0.1 to 1.9
- mix_weight: bfloat16 [2048, 14336], P(None, 'head'), may hold values from -0.125 to 0.125
- rate_weight: bfloat16 [2048, 64], P(None, 'head'), may hold values from -0.5524272 to 0.5524272
- decay_rate: float32 [16], P('head'), may hold values from 0.0005 to 0.03
- head_gain: float32 [128], replicated, may hold values from 0.1 to 1.9
- out_weight: bfloat16 [2048, 2048], P('head'), may hold values from -0.125 to 0.125
- final_gain: float32 [2048], replicated, may hold values from 0.1 to 1.9
- vocab_table: bfloat16 [16384, 2048], P(('batch', 'head')), may hold values from -50.8233 to 50.8233
- next_token: int32 [32], replicated, may hold values from 0 to 16383
Outputs:
- mixed: bfloat16 [4096, 2048], P('batch', 'head')
- new_state: float32 [32, 16, 128, 128], P('batch', 'head')
- log_likelihood: float32 [32], replicated
The draws below stay inside these ranges and needn't reach their ends.
All inputs are finite; a program needn't handle non-finite values.
Results may differ from the reference program's by a relative error of at most 0.0058.
The reference program's roundings to bfloat16 on the way count: a program that leaves them out, or rounds other values in their place, can miss the bound.
Values may be sent and summed in bfloat16 or wider, within the bound.
A program may use at most 128 MiB of HBM per device.

```python
import math
import jax
import jax.numpy as jnp
import numpy as np
from jax import lax

D = 2048
HEADS = 16
HEAD_DIM = 128
REFLECT = 3
VOCAB = 16384
NEW_POSITIONS = 128
SEQUENCE_COUNT = 32
TOKEN_ROWS_ALL = 4096


def householder_directions(key):
    reflect_vectors = jnp.clip(jax.random.normal(jax.random.fold_in(key, 101), (D, HEADS), jnp.float32), -4.0, 4.0)
    return reflect_vectors / jnp.sqrt(1.0 * D)


def draw_tokens(key, part):
    reflect_vectors = householder_directions(key)
    shared_way = jnp.sum(reflect_vectors, axis=1)
    shared_way = shared_way / jnp.sqrt(jnp.sum(shared_way * shared_way))
    column_scale = 0.3 * 10.0 ** (jnp.arange(D, dtype=jnp.float32) / (D - 1))
    row_scale = 10.0 ** jax.random.uniform(jax.random.fold_in(key, 102), (TOKEN_ROWS_ALL, 1), jnp.float32, -1.0, 0.0)
    base = jnp.clip(jax.random.normal(jax.random.fold_in(key, 103), (TOKEN_ROWS_ALL, D), jnp.float32), -4.0, 4.0)
    values = base * row_scale * column_scale
    householder_steps = jax.random.randint(jax.random.fold_in(key, 105), (SEQUENCE_COUNT, 2), 0, NEW_POSITIONS)
    position_places = jnp.arange(NEW_POSITIONS)
    masked_entries = jnp.any(position_places[None, :, None] == householder_steps[:, None, :], axis=2).reshape(TOKEN_ROWS_ALL, 1)
    values = values + jnp.where(masked_entries, 80.0 * shared_way[None, :], 0.0)
    return values.astype(jnp.bfloat16)


def draw_rate_weight(key, part):
    reflect_vectors = householder_directions(key)
    noise = jnp.clip(jax.random.normal(jax.random.fold_in(key, 111), (D, HEADS, REFLECT + 1), jnp.float32), -5.0, 5.0)
    noise = noise / jnp.sqrt(1.0 * D)
    boost = jnp.concatenate([jnp.zeros((D, HEADS, REFLECT), jnp.float32), 5.0 * reflect_vectors[:, :, None]], axis=2)
    return (noise + boost).reshape(D, HEADS * (REFLECT + 1)).astype(jnp.bfloat16)


def draw_decay_rate(key, part):
    spread = jax.random.uniform(jax.random.fold_in(key, 121), (HEADS,), jnp.float32)
    rates = 0.002 * 15.0 ** spread
    return rates


def draw_vocab_table(key, part):
    row_scale = 10.0 ** jax.random.uniform(jax.random.fold_in(key, 131), (VOCAB, 1), jnp.float32)
    base = jnp.clip(jax.random.normal(jax.random.fold_in(key, 132), (VOCAB, D), jnp.float32), -5.0, 5.0)
    values = base * row_scale / jnp.sqrt(1.0 * D)
    return values.astype(jnp.bfloat16)


def touch_ends(values, own_key, least, high):
    extent = values.shape
    index_at = [jax.random.randint(jax.random.fold_in(own_key, axis), (), 0, extent[axis]) for axis in range(len(extent))]
    values = values.at[tuple(index_at)].set(least)
    longest = extent.index(max(extent))
    index_at[longest] = (index_at[longest] + 1) % extent[longest]
    return values.at[tuple(index_at)].set(high)


def level_of(own_key, dims, split, smallest, top_value):
    gain, own = 1.0, jax.random.fold_in(own_key, 6)
    for axis_at, blocks in split:
        heights = jnp.exp(jax.random.uniform(jax.random.fold_in(own, axis_at), (blocks,), jnp.float32, smallest / len(split), top_value / len(split)))
        gain = gain * jnp.repeat(heights, dims[axis_at] // blocks).reshape([-1 if axis == axis_at else 1 for axis in range(len(dims))])
    return gain


def rank_bounds(amount, slope):
    loads = [(1 << 20) // math.isqrt(rank ** slope) + 1 for rank in range(1, amount + 1)]
    scale = 1 + sum(loads) // (1 << 30)
    return np.cumsum(np.array([max(1, weight // scale) for weight in loads]))


def ranked(key, shape, number_of, slope):
    table = rank_bounds(number_of, slope)
    ticket = jax.random.randint(jax.random.fold_in(key, 1), shape, 0, int(table[number_of - 1]))
    standing = jnp.searchsorted(jnp.asarray(table, jnp.int32), ticket, side="right")
    return jax.random.permutation(jax.random.fold_in(key, 2), number_of)[standing].astype(jnp.int32)


def bell_draw(stream_key, shape, scale, most, cuts=(), kind=jnp.bfloat16):
    drawn = jax.random.normal(stream_key, shape, jnp.float32) * scale
    if len(cuts) > 0:
        drawn = level_of(stream_key, shape, cuts, -0.22, 0.18) * drawn
    return jnp.clip(drawn, min=-most, max=most).astype(kind)


def setup_inputs(seed: int = 0) -> dict:
    streams_of = jax.random.split(jax.random.key(seed), 13)
    tokens = draw_tokens(jax.random.fold_in(streams_of[12], 71), 0)
    lengths = touch_ends(jax.random.randint(streams_of[1], (SEQUENCE_COUNT,), 1, NEW_POSITIONS + 1), jax.random.fold_in(streams_of[1], 1), 1, NEW_POSITIONS).astype(jnp.int32)
    states = bell_draw(streams_of[2], (SEQUENCE_COUNT, HEADS, HEAD_DIM, HEAD_DIM), 0.5, 3.0, ((0, 8), (1, 4)), jnp.float32)
    norm_gain = jnp.clip(1.0 + 0.18 * jax.random.normal(streams_of[3], (D,), jnp.float32), 0.1, 1.9)
    mix_weight = bell_draw(streams_of[4], (D, HEADS * (2 * REFLECT + 1) * HEAD_DIM), D ** -0.5, 0.125, ((1, 4),))
    rate_weight = draw_rate_weight(jax.random.fold_in(streams_of[12], 71), 0)
    decay_rate = draw_decay_rate(jax.random.fold_in(streams_of[12], 71), 0)
    head_gain = jnp.clip(1.0 + 0.18 * jax.random.normal(streams_of[7], (HEAD_DIM,), jnp.float32), 0.1, 1.9)
    out_weight = bell_draw(streams_of[8], (HEADS * HEAD_DIM, D), (HEADS * HEAD_DIM) ** -0.5, 0.125, ((0, 4),))
    final_gain = jnp.clip(1.0 + 0.18 * jax.random.normal(streams_of[9], (D,), jnp.float32), 0.1, 1.9)
    vocab_table = draw_vocab_table(jax.random.fold_in(streams_of[12], 71), 0)
    next_token = touch_ends(ranked(streams_of[11], (SEQUENCE_COUNT,), VOCAB, 2), jax.random.fold_in(streams_of[11], 3), 0, VOCAB - 1).astype(jnp.int32)
    return dict(tokens=tokens, lengths=lengths, states=states, norm_gain=norm_gain, mix_weight=mix_weight, rate_weight=rate_weight, decay_rate=decay_rate, head_gain=head_gain, out_weight=out_weight, final_gain=final_gain, vocab_table=vocab_table, next_token=next_token)


ROW_EPSILON = 1e-05
KEY_EPSILON = 1e-06
HIGHEST_PRECISION = lax.Precision.HIGHEST

def delta_block(queries, key_rows, value_rows, beta_rows, log_decay, start_state):
    positions = key_rows.shape[0]
    reflections = key_rows.shape[1]
    total_steps = positions * reflections
    flat_keys = key_rows.reshape(total_steps, key_rows.shape[2])
    flat_values = value_rows.reshape(total_steps, value_rows.shape[2])
    flat_betas = beta_rows.reshape(total_steps)
    padding = jnp.zeros((positions, reflections - 1), log_decay.dtype)
    step_decay = jnp.concatenate([log_decay[:, None], padding], axis=1).reshape(total_steps)
    cumulative = jnp.cumsum(step_decay)
    step_index = jnp.arange(total_steps)
    earlier = step_index[:, None] > step_index[None, :]
    decay_ratio = jnp.exp(jnp.where(earlier, cumulative[:, None] - cumulative[None, :], -jnp.inf))
    key_gram = jnp.dot(flat_keys, flat_keys.T, precision=HIGHEST_PRECISION)
    system = jnp.eye(total_steps, dtype=key_gram.dtype) + flat_betas[:, None] * decay_ratio * key_gram
    start_image = jnp.dot(flat_keys, start_state.T, precision=HIGHEST_PRECISION)
    source = flat_betas[:, None] * (flat_values - jnp.exp(cumulative)[:, None] * start_image)
    updates = jax.scipy.linalg.solve_triangular(system, source, lower=True, unit_diagonal=True)
    query_cumulative = cumulative.reshape(positions, reflections)[:, reflections - 1]
    query_step = step_index.reshape(positions, reflections)[:, reflections - 1]
    visible = step_index[None, :] <= query_step[:, None]
    weights = jnp.exp(jnp.where(visible, query_cumulative[:, None] - cumulative[None, :], -jnp.inf))
    scores = jnp.dot(queries, flat_keys.T, precision=HIGHEST_PRECISION) * weights
    attended = jnp.exp(query_cumulative)[:, None] * jnp.dot(queries, start_state.T, precision=HIGHEST_PRECISION)
    attended = attended + jnp.dot(scores, updates, precision=HIGHEST_PRECISION)
    tail_decay = jnp.exp(cumulative[total_steps - 1] - cumulative)
    new_state = jnp.exp(cumulative[total_steps - 1]) * start_state
    new_state = new_state + jnp.dot(updates.T, tail_decay[:, None] * flat_keys, precision=HIGHEST_PRECISION)
    return (attended, new_state)

def head_inputs(projected, rate_logits, valid_mask, decay_rate):
    queries = jax.nn.silu(projected[:, :, :, 0])
    key_rows = jax.nn.silu(projected[:, :, :, 1:REFLECT + 1])
    key_rows = key_rows * lax.rsqrt(lax.optimization_barrier(jnp.sum(key_rows * key_rows, axis=-1, keepdims=True)) + KEY_EPSILON)
    value_rows = jax.nn.silu(projected[:, :, :, REFLECT + 1:])
    beta_rows = jnp.where(valid_mask[:, :, None, None], 2.0 * jax.nn.sigmoid(rate_logits[..., :REFLECT]), 0.0)
    log_decay = jnp.where(valid_mask[:, :, None], -decay_rate * jax.nn.softplus(rate_logits[..., REFLECT]), 0.0)
    return (queries, key_rows, value_rows, beta_rows, log_decay)

def run_heads(queries, key_rows, value_rows, beta_rows, log_decay, start_states):
    per_head = jax.vmap(delta_block, in_axes=(1, 1, 1, 1, 1, 0), out_axes=(1, 0))
    per_sequence = jax.vmap(per_head)
    return per_sequence(queries, key_rows, value_rows, beta_rows, log_decay, start_states)

def head_norm(attended, head_gain):
    factor = lax.rsqrt(lax.optimization_barrier(jnp.mean(attended * attended, axis=-1, keepdims=True)) + ROW_EPSILON)
    return (attended * factor * head_gain).astype(jnp.bfloat16)

def reference(tokens, lengths, states, norm_gain, mix_weight, rate_weight, decay_rate, head_gain, out_weight, final_gain, vocab_table, next_token):
    model_width = tokens.shape[1]
    blocks = tokens.reshape(lengths.shape[0], NEW_POSITIONS, model_width)

    def one_sequence(inputs):
        block_rows, length, start_state = inputs
        widened = block_rows.astype(jnp.float32)
        scaled = (widened * norm_gain).astype(jnp.bfloat16)
        inverse = lax.rsqrt(lax.optimization_barrier(jnp.mean(widened * widened, axis=1, keepdims=True)) + ROW_EPSILON)
        projected = jnp.dot(scaled.astype(jnp.float32), mix_weight.astype(jnp.float32), preferred_element_type=jnp.float32) * inverse
        rate_logits = jnp.dot(scaled.astype(jnp.float32), rate_weight.astype(jnp.float32), preferred_element_type=jnp.float32) * inverse
        projected = projected.reshape(1, NEW_POSITIONS, HEADS, 2 * REFLECT + 1, HEAD_DIM)
        rate_logits = rate_logits.reshape(1, NEW_POSITIONS, HEADS, REFLECT + 1)
        valid_mask = (jnp.arange(NEW_POSITIONS) < length)[None, :]
        queries, key_rows, value_rows, beta_rows, log_decay = head_inputs(projected, rate_logits, valid_mask, decay_rate)
        attended, new_state = run_heads(queries, key_rows, value_rows, beta_rows, log_decay, start_state[None])
        normed = head_norm(attended, head_gain).reshape(NEW_POSITIONS, HEADS * HEAD_DIM)
        mixed = (widened + jnp.dot(normed.astype(jnp.float32), out_weight.astype(jnp.float32), preferred_element_type=jnp.float32)).astype(jnp.bfloat16)
        last_row = lax.dynamic_slice_in_dim(mixed, (length - 1).astype(jnp.int32), 1, 0)[0]
        return (mixed, new_state[0], last_row)
    mixed, new_state, last_rows = lax.map(one_sequence, (blocks, lengths, states))
    widened = last_rows.astype(jnp.float32)
    factor = lax.rsqrt(lax.optimization_barrier(jnp.mean(widened * widened, axis=1, keepdims=True)) + ROW_EPSILON)
    hidden = (widened * factor * final_gain).astype(jnp.bfloat16)
    logits = jnp.dot(hidden.astype(jnp.float32), vocab_table.T.astype(jnp.float32), preferred_element_type=jnp.float32)
    largest = lax.optimization_barrier(jnp.max(logits, axis=1))
    exp_total = lax.optimization_barrier(jnp.sum(jnp.exp(logits - largest[:, None]), axis=1))
    target = jnp.take_along_axis(logits, next_token[:, None], axis=1)[:, 0]
    log_likelihood = target - (largest + jnp.log(exp_total))
    return (mixed.reshape(tokens.shape), new_state, log_likelihood)
```

```python
import functools
import jax
import jax.numpy as jnp
from jax import lax
from jax.experimental import pallas as pl
from jax.experimental.pallas import tpu as pltpu
from jax.sharding import PartitionSpec as P

HEAD_DIM = 128
REFLECT = 3
NEW_POSITIONS = 128
STEPS = NEW_POSITIONS * REFLECT
BLOCK = 128

ROW_EPSILON = 1e-05
KEY_EPSILON = 1e-06
MESH = pl.DeviceIdType.MESH
F32 = jnp.float32
BF16 = jnp.bfloat16


def halves(x):
    high = x.astype(BF16)
    low = (x - high.astype(F32)).astype(BF16)
    return high, low


def left_side(x):
    return jnp.concatenate(halves(x), axis=1)


def right_side(x):
    row = jnp.concatenate(halves(x), axis=1)
    return jnp.concatenate([row, row], axis=0)


def right_transposed(x):
    high, low = halves(x)
    return jnp.concatenate(
        [jnp.concatenate([high, high], axis=1), jnp.concatenate([low, low], axis=1)], axis=0
    )


def folded(both):
    width = both.shape[1] // 2
    return both[:, :width] + both[:, width:]


def mm(left, right):
    return folded(jnp.dot(left, right, preferred_element_type=F32))


def mm_t(left, right):
    return folded(
        lax.dot_general(left, right, (((1,), (1,)), ((), ())), preferred_element_type=F32)
    )


def silu(x):
    return x / (1.0 + jnp.exp(-x))


def mixer_kernel(
    heads,
    lengths_ref,
    decay_ref,
    proj_ref,
    inverse_ref,
    rates_ref,
    gain_ref,
    state_ref,
    normed_ref,
    new_state_ref,
    keys_ref,
    scaled_keys_ref,
    scaled_values_ref,
):
    sequence = pl.program_id(0)
    group = pl.program_id(1)
    length = lengths_ref[sequence]
    inverse = inverse_ref[...]
    position = lax.broadcasted_iota(jnp.int32, (NEW_POSITIONS, 1), 0)
    valid = position < length
    rates = rates_ref[0] * inverse
    blocks = STEPS // BLOCK
    row_id = lax.broadcasted_iota(jnp.int32, (BLOCK, BLOCK), 0)
    col_id = lax.broadcasted_iota(jnp.int32, (BLOCK, BLOCK), 1)
    step_row = lax.broadcasted_iota(jnp.int32, (STEPS, NEW_POSITIONS), 0)
    step_col = lax.broadcasted_iota(jnp.int32, (STEPS, NEW_POSITIONS), 1)
    summing = jnp.concatenate(
        [
            jnp.where(step_col * REFLECT <= step_row, 1.0, 0.0).astype(F32),
            jnp.where(col_id <= row_id, 1.0, 0.0).astype(F32),
        ],
        axis=0,
    )
    queries, decays = [], []
    for i in range(heads):
        base = i * (2 * REFLECT + 1) * HEAD_DIM

        def part(k):
            start = base + k * HEAD_DIM
            return silu(proj_ref[:, start : start + HEAD_DIM] * inverse)

        queries.append(part(0))
        for j in range(REFLECT):
            rate = i * (REFLECT + 1)
            beta = jnp.where(
                valid, 2.0 / (1.0 + jnp.exp(-rates[:, rate + j : rate + j + 1])), 0.0
            )
            key = part(1 + j)
            key = key * lax.rsqrt(jnp.sum(key * key, axis=1, keepdims=True) + KEY_EPSILON)
            places = pl.ds(j, NEW_POSITIONS, REFLECT)
            keys_ref.at[i][places, :] = key
            scaled_keys_ref.at[i][places, :] = key * beta
            scaled_values_ref.at[i][places, :] = part(1 + REFLECT + j) * beta
        logit = rates[:, i * (REFLECT + 1) + REFLECT : (i + 1) * (REFLECT + 1)]
        softplus = jnp.maximum(logit, 0.0) + jnp.log1p(jnp.exp(-jnp.abs(logit)))
        rate_here = decay_ref[group * heads + i]
        log_decay = jnp.where(valid, -rate_here * softplus, 0.0)
        decays.append(
            jnp.dot(
                summing,
                jnp.broadcast_to(log_decay, (NEW_POSITIONS, HEAD_DIM)),
                preferred_element_type=F32,
                precision=lax.Precision.HIGHEST,
            )
        )

    def rows(x, b):
        return x[b * BLOCK : (b + 1) * BLOCK]

    lower, inverses, scores, sources, carried, tails, flipped = {}, {}, {}, {}, [], [], {}
    for i in range(heads):
        decay_column = decays[i]
        query_decay = decay_column[STEPS:]
        left_scaled = left_side(scaled_keys_ref[i])
        left_query = left_side(queries[i])
        start = right_transposed(state_ref[0, i])
        image = mm_t(left_scaled, start)
        grown = jnp.exp(decay_column[:STEPS])
        source = scaled_values_ref[i] - grown * image
        carried.append(jnp.exp(query_decay) * mm_t(left_query, start))
        last = query_decay[NEW_POSITIONS - 1 :]
        tail = jnp.exp(last - decay_column[:STEPS])
        tails.append((jnp.exp(last), tail * keys_ref[i]))
        for b in range(blocks):
            sources[i, b] = rows(source, b)
            flip = rows(decay_column, b).T
            right = right_transposed(keys_ref[i, b * BLOCK : (b + 1) * BLOCK, :])
            for a in range(b, blocks):
                gram = mm_t(rows(left_scaled, a), right)
                ratio = jnp.exp(jnp.minimum(rows(decay_column, a) - flip, 0.0))
                value = gram * ratio
                if a == b:
                    value = jnp.where(row_id > col_id, value, 0.0)
                lower[i, a, b] = value
            seen = b * BLOCK + col_id < (row_id + 1) * REFLECT
            weight = jnp.exp(jnp.minimum(query_decay - flip, 0.0))
            scores[i, b] = jnp.where(seen, mm_t(left_query, right) * weight, 0.0)

    chains = [(i, b) for i in range(heads) for b in range(blocks)]
    differ = row_id ^ col_id
    identity = jnp.where(row_id == col_id, 1.0, 0.0).astype(F32)
    for chain in chains:
        i, b = chain
        inverses[chain] = identity - jnp.where(differ == 1, lower[i, b, b], 0.0)
    level = 1
    while (1 << level) < BLOCK:
        crossing = (differ >> level) == 1
        for chain in chains:
            i, b = chain
            x = inverses[chain]
            border = right_side(jnp.where(crossing, lower[i, b, b], 0.0))
            first = mm(left_side(x), border)
            inverses[chain] = x - mm(left_side(first), right_side(x))
        level += 1

    updates = {}
    for b in range(blocks):
        for i in range(heads):
            source = sources[i, b]
            for a in range(b):
                source = source - mm(left_side(lower[i, b, a]), updates[i, a])
            update = mm(left_side(inverses[i, b]), right_side(source))
            updates[i, b] = right_side(update)
            grown, _ = tails[i]
            carried[i] = carried[i] + mm(left_side(scores[i, b]), updates[i, b])
            sources[i, b] = update
    for i in range(heads):
        factor = lax.rsqrt(
            jnp.mean(carried[i] * carried[i], axis=1, keepdims=True) + ROW_EPSILON
        )
        normed_ref[:, i * HEAD_DIM : (i + 1) * HEAD_DIM] = (
            carried[i] * factor * gain_ref[...]
        ).astype(BF16)
        grown, tail = tails[i]
        total = grown * state_ref[0, i]
        for b in range(blocks):
            total = total + mm(left_side(sources[i, b].T), right_side(rows(tail, b)))
        new_state_ref[0, i] = total


def mixer(projected, inverse, rate_logits, lengths, decay_rate, head_gain, states):
    sequences, local_heads = states.shape[0], states.shape[1]
    heads = 2 if local_heads % 2 == 0 else 1
    groups = local_heads // heads
    local_rows = projected.shape[0]
    per_head = REFLECT + 1
    rates = rate_logits.reshape(local_rows, groups, heads * per_head).transpose(1, 0, 2)
    wide = heads * (2 * REFLECT + 1) * HEAD_DIM
    smem = pl.BlockSpec(memory_space=pltpu.SMEM)
    state_spec = pl.BlockSpec((1, heads, HEAD_DIM, HEAD_DIM), lambda s, g: (s, g, 0, 0))
    steps = pltpu.VMEM((heads, STEPS, HEAD_DIM), F32)
    return pl.pallas_call(
        functools.partial(mixer_kernel, heads),
        grid=(sequences, groups),
        in_specs=[
            smem,
            smem,
            pl.BlockSpec((NEW_POSITIONS, wide), lambda s, g: (s, g)),
            pl.BlockSpec((NEW_POSITIONS, 1), lambda s, g: (s, 0)),
            pl.BlockSpec((1, NEW_POSITIONS, heads * per_head), lambda s, g: (g, s, 0)),
            pl.BlockSpec((1, HEAD_DIM), lambda s, g: (0, 0)),
            state_spec,
        ],
        out_specs=[
            pl.BlockSpec((NEW_POSITIONS, heads * HEAD_DIM), lambda s, g: (s, g)),
            state_spec,
        ],
        out_shape=[
            jax.ShapeDtypeStruct((local_rows, local_heads * HEAD_DIM), BF16),
            jax.ShapeDtypeStruct(states.shape, F32),
        ],
        scratch_shapes=[steps, steps, steps],
        name="mixer",
    )(lengths, decay_rate, projected, inverse, rates, head_gain[None], states)


def tail_kernel(
    batch_count,
    head_count,
    last_ref,
    gain_ref,
    table_hbm,
    next_ref,
    out_ref,
    table_ref,
    rows_ref,
    wide_ref,
    own_ref,
    stats_ref,
    table_sem,
    row_send,
    row_recv,
    stat_send,
    stat_recv,
):
    count = batch_count * head_count
    batch_at, head_at = lax.axis_index("batch"), lax.axis_index("head")
    me = batch_at * head_count + head_at
    sequences, width = last_ref.shape
    vocab_here = table_ref.shape[0]

    load = pltpu.make_async_copy(table_hbm, table_ref, table_sem)
    load.start()

    def other(k):
        index = lax.rem(me + k, count)
        return index, {"batch": index // head_count, "head": lax.rem(index, head_count)}

    barrier = pltpu.get_barrier_semaphore()

    @pl.loop(1, count)
    def _(k):
        pl.semaphore_signal(barrier, inc=1, device_id=other(k)[1], device_id_type=MESH)

    pl.semaphore_wait(barrier, count - 1)

    def row_copy(k, slot):
        return pltpu.make_async_remote_copy(
            src_ref=last_ref,
            dst_ref=rows_ref.at[slot],
            send_sem=row_send.at[k],
            recv_sem=row_recv.at[slot],
            device_id=other(k)[1],
            device_id_type=MESH,
        )

    @pl.loop(1, count)
    def _(k):
        row_copy(k, me).start()

    rows_ref[me] = last_ref[...]

    @pl.loop(1, count)
    def _(k):
        row_copy(k, other(k)[0]).wait_recv()

    for b in range(batch_count):
        for h in range(head_count):
            wide_ref[b * sequences : (b + 1) * sequences, h * width : (h + 1) * width] = rows_ref[
                b * head_count + h
            ].astype(F32)
    everyone = wide_ref[...]
    factor = lax.rsqrt(jnp.mean(everyone * everyone, axis=1, keepdims=True) + ROW_EPSILON)
    hidden = (everyone * factor * gain_ref[...]).astype(BF16)
    load.wait()
    logits = lax.dot_general(
        table_ref[...], hidden, (((1,), (1,)), ((), ())), preferred_element_type=F32
    )
    ids = lax.broadcasted_iota(jnp.int32, logits.shape, 0) + me * vocab_here
    largest = jnp.max(logits, axis=0, keepdims=True)
    own_ref[0:1, :] = largest
    own_ref[1:2, :] = jnp.sum(jnp.exp(logits - largest), axis=0, keepdims=True)
    own_ref[2:3, :] = jnp.sum(
        jnp.where(ids == next_ref[...], logits, 0.0), axis=0, keepdims=True
    )
    own_ref[3:, :] = jnp.zeros((own_ref.shape[0] - 3, own_ref.shape[1]), F32)

    def stat_copy(k, slot):
        return pltpu.make_async_remote_copy(
            src_ref=own_ref,
            dst_ref=stats_ref.at[slot],
            send_sem=stat_send.at[k],
            recv_sem=stat_recv.at[slot],
            device_id=other(k)[1],
            device_id_type=MESH,
        )

    @pl.loop(1, count)
    def _(k):
        stat_copy(k, me).start()

    stats_ref[me] = own_ref[...]

    @pl.loop(1, count)
    def _(k):
        row_copy(k, me).wait_send()
        stat_copy(k, other(k)[0]).wait_recv()

    highest = lax.fori_loop(
        0, count, lambda d, top: jnp.maximum(top, stats_ref[d][0:1]), largest
    )

    def add(d, totals):
        entry = stats_ref[d]
        return (totals[0] + entry[1:2] * jnp.exp(entry[0:1] - highest), totals[1] + entry[2:3])

    zero = jnp.zeros_like(largest)
    summed, target = lax.fori_loop(0, count, add, (zero, zero))
    out_ref[...] = target - (highest + jnp.log(summed))

    @pl.loop(1, count)
    def _(k):
        stat_copy(k, me).wait_send()


def tail(last_rows, final_gain, vocab_table, next_token):
    batch_count, head_count = lax.axis_size("batch"), lax.axis_size("head")
    count = batch_count * head_count
    sequences, width = last_rows.shape
    everyone = next_token.shape[0]
    vmem = pl.BlockSpec(memory_space=pltpu.VMEM)
    semaphores = pltpu.SemaphoreType.DMA((count,))
    return pl.pallas_call(
        functools.partial(tail_kernel, batch_count, head_count),
        out_shape=jax.ShapeDtypeStruct((1, everyone), F32),
        in_specs=[vmem, vmem, pl.BlockSpec(memory_space=pl.ANY), vmem],
        out_specs=vmem,
        scratch_shapes=[
            pltpu.VMEM(vocab_table.shape, BF16),
            pltpu.VMEM((count, sequences, width), BF16),
            pltpu.VMEM((everyone, final_gain.shape[0]), F32),
            pltpu.VMEM((8, everyone), F32),
            pltpu.VMEM((count, 8, everyone), F32),
            pltpu.SemaphoreType.DMA,
            semaphores,
            semaphores,
            semaphores,
            semaphores,
        ],
        compiler_params=pltpu.CompilerParams(collective_id=1, has_side_effects=True),
        name="tail",
    )(last_rows, final_gain[None], vocab_table, next_token[None])[0]


def on_device(
    tokens,
    lengths,
    states,
    norm_gain,
    mix_weight,
    rate_weight,
    decay_rate,
    head_gain,
    out_weight,
    final_gain,
    vocab_table,
    next_token,
):
    sequences = lengths.shape[0]
    local_width = tokens.shape[1]
    model_width = norm_gain.shape[0]
    wide = lax.all_gather(tokens, "head", axis=1, tiled=True).astype(F32)
    scaled = (wide * norm_gain).astype(BF16)
    inverse = lax.rsqrt(jnp.sum(wide * wide, axis=1, keepdims=True) / model_width + ROW_EPSILON)
    projected = jnp.dot(scaled, mix_weight, preferred_element_type=F32)
    rate_logits = jnp.dot(scaled, rate_weight, preferred_element_type=F32)
    normed, new_state = mixer(
        projected, inverse, rate_logits, lengths, decay_rate, head_gain, states
    )
    mix_sum = lax.psum_scatter(
        lax.dot_general(
            out_weight, normed, (((0,), (1,)), ((), ())), preferred_element_type=F32
        ),
        "head",
        scatter_dimension=0,
        tiled=True,
    ).T
    mixed = (tokens.astype(F32) + mix_sum).astype(BF16)
    last_index = (lengths - 1)[:, None, None]
    last_rows = jnp.take_along_axis(
        mixed.reshape(sequences, NEW_POSITIONS, local_width), last_index, axis=1
    )[:, 0]
    log_likelihood = tail(last_rows, final_gain, vocab_table, next_token)
    return (mixed, new_state, log_likelihood)


def solution(mesh):
    placed = (
        P("batch", "head"),
        P("batch"),
        P("batch", "head", None, None),
        P(),
        P(None, "head"),
        P(None, "head"),
        P("head"),
        P(),
        P("head", None),
        P(),
        P(("batch", "head"), None),
        P(),
    )
    return jax.shard_map(
        on_device,
        mesh=mesh,
        in_specs=placed,
        out_specs=(P("batch", "head"), P("batch", "head", None, None), P()),
        check_vma=False,
    )
```

```python
import functools
import jax
import jax.numpy as jnp
from jax import lax
from jax.experimental import pallas as pl
from jax.experimental.pallas import tpu as pltpu
from jax.sharding import PartitionSpec as P

HEAD_DIM = 128
REFLECT = 3
NEW_POSITIONS = 128
STEPS = NEW_POSITIONS * REFLECT
BLOCK = 128
PIECES = 2

ROW_EPSILON = 1e-05
KEY_EPSILON = 1e-06
MESH = pl.DeviceIdType.MESH
F32 = jnp.float32
BF16 = jnp.bfloat16


def halves(x):
    high = x.astype(BF16)
    low = (x - high.astype(F32)).astype(BF16)
    return high, low


def left_side(x):
    return jnp.concatenate(halves(x), axis=1)


def right_side(x):
    row = jnp.concatenate(halves(x), axis=1)
    return jnp.concatenate([row, row], axis=0)


def right_transposed(x):
    high, low = halves(x)
    return jnp.concatenate(
        [jnp.concatenate([high, high], axis=1), jnp.concatenate([low, low], axis=1)], axis=0
    )


def folded(both):
    width = both.shape[1] // 2
    return both[:, :width] + both[:, width:]


def mm(left, right):
    return folded(jnp.dot(left, right, preferred_element_type=F32))


def mm_t(left, right):
    return folded(
        lax.dot_general(left, right, (((1,), (1,)), ((), ())), preferred_element_type=F32)
    )


def silu(x):
    return x / (1.0 + jnp.exp(-x))


def mixer_kernel(
    heads,
    lengths_ref,
    decay_ref,
    proj_ref,
    inverse_ref,
    rates_ref,
    gain_ref,
    state_ref,
    normed_ref,
    new_state_ref,
    keys_ref,
    scaled_keys_ref,
    scaled_values_ref,
):
    sequence = pl.program_id(0)
    group = pl.program_id(1)
    length = lengths_ref[sequence]
    inverse = inverse_ref[...]
    position = lax.broadcasted_iota(jnp.int32, (NEW_POSITIONS, 1), 0)
    valid = position < length
    rates = rates_ref[0] * inverse
    blocks = STEPS // BLOCK
    row_id = lax.broadcasted_iota(jnp.int32, (BLOCK, BLOCK), 0)
    col_id = lax.broadcasted_iota(jnp.int32, (BLOCK, BLOCK), 1)
    step_row = lax.broadcasted_iota(jnp.int32, (STEPS, NEW_POSITIONS), 0)
    step_col = lax.broadcasted_iota(jnp.int32, (STEPS, NEW_POSITIONS), 1)
    summing = jnp.concatenate(
        [
            jnp.where(step_col * REFLECT <= step_row, 1.0, 0.0).astype(F32),
            jnp.where(col_id <= row_id, 1.0, 0.0).astype(F32),
        ],
        axis=0,
    )
    queries, decays = [], []
    for i in range(heads):
        base = i * (2 * REFLECT + 1) * HEAD_DIM

        def part(k):
            start = base + k * HEAD_DIM
            return silu(proj_ref[:, start : start + HEAD_DIM] * inverse)

        queries.append(part(0))
        for j in range(REFLECT):
            rate = i * (REFLECT + 1)
            beta = jnp.where(
                valid, 2.0 / (1.0 + jnp.exp(-rates[:, rate + j : rate + j + 1])), 0.0
            )
            key = part(1 + j)
            key = key * lax.rsqrt(jnp.sum(key * key, axis=1, keepdims=True) + KEY_EPSILON)
            places = pl.ds(j, NEW_POSITIONS, REFLECT)
            keys_ref.at[i][places, :] = key
            scaled_keys_ref.at[i][places, :] = key * beta
            scaled_values_ref.at[i][places, :] = part(1 + REFLECT + j) * beta
        logit = rates[:, i * (REFLECT + 1) + REFLECT : (i + 1) * (REFLECT + 1)]
        softplus = jnp.maximum(logit, 0.0) + jnp.log1p(jnp.exp(-jnp.abs(logit)))
        rate_here = decay_ref[group * heads + i]
        log_decay = jnp.where(valid, -rate_here * softplus, 0.0)
        decays.append(
            jnp.dot(
                summing,
                jnp.broadcast_to(log_decay, (NEW_POSITIONS, HEAD_DIM)),
                preferred_element_type=F32,
                precision=lax.Precision.HIGHEST,
            )
        )

    def rows(x, b):
        return x[b * BLOCK : (b + 1) * BLOCK]

    lower, inverses, scores, sources, carried, tails, flipped = {}, {}, {}, {}, [], [], {}
    for i in range(heads):
        decay_column = decays[i]
        query_decay = decay_column[STEPS:]
        left_scaled = left_side(scaled_keys_ref[i])
        left_query = left_side(queries[i])
        start = right_transposed(state_ref[0, i])
        image = mm_t(left_scaled, start)
        grown = jnp.exp(decay_column[:STEPS])
        source = scaled_values_ref[i] - grown * image
        carried.append(jnp.exp(query_decay) * mm_t(left_query, start))
        last = query_decay[NEW_POSITIONS - 1 :]
        tail = jnp.exp(last - decay_column[:STEPS])
        tails.append((jnp.exp(last), tail * keys_ref[i]))
        for b in range(blocks):
            sources[i, b] = rows(source, b)
            flip = rows(decay_column, b).T
            right = right_transposed(keys_ref[i, b * BLOCK : (b + 1) * BLOCK, :])
            for a in range(b, blocks):
                gram = mm_t(rows(left_scaled, a), right)
                ratio = jnp.exp(jnp.minimum(rows(decay_column, a) - flip, 0.0))
                value = gram * ratio
                if a == b:
                    value = jnp.where(row_id > col_id, value, 0.0)
                lower[i, a, b] = value
            seen = b * BLOCK + col_id < (row_id + 1) * REFLECT
            weight = jnp.exp(jnp.minimum(query_decay - flip, 0.0))
            scores[i, b] = jnp.where(seen, mm_t(left_query, right) * weight, 0.0)

    chains = [(i, b) for i in range(heads) for b in range(blocks)]
    differ = row_id ^ col_id
    identity = jnp.where(row_id == col_id, 1.0, 0.0).astype(F32)
    for chain in chains:
        i, b = chain
        inverses[chain] = identity - jnp.where(differ == 1, lower[i, b, b], 0.0)
    level = 1
    while (1 << level) < BLOCK:
        crossing = (differ >> level) == 1
        for chain in chains:
            i, b = chain
            x = inverses[chain]
            border = right_side(jnp.where(crossing, lower[i, b, b], 0.0))
            first = mm(left_side(x), border)
            inverses[chain] = x - mm(left_side(first), right_side(x))
        level += 1

    updates = {}
    for b in range(blocks):
        for i in range(heads):
            source = sources[i, b]
            for a in range(b):
                source = source - mm(left_side(lower[i, b, a]), updates[i, a])
            update = mm(left_side(inverses[i, b]), right_side(source))
            updates[i, b] = right_side(update)
            grown, _ = tails[i]
            carried[i] = carried[i] + mm(left_side(scores[i, b]), updates[i, b])
            sources[i, b] = update
    for i in range(heads):
        factor = lax.rsqrt(
            jnp.mean(carried[i] * carried[i], axis=1, keepdims=True) + ROW_EPSILON
        )
        normed_ref[:, i * HEAD_DIM : (i + 1) * HEAD_DIM] = (
            carried[i] * factor * gain_ref[...]
        ).astype(BF16)
        grown, tail = tails[i]
        total = grown * state_ref[0, i]
        for b in range(blocks):
            total = total + mm(left_side(sources[i, b].T), right_side(rows(tail, b)))
        new_state_ref[0, i] = total


def mixer(projected, inverse, rate_logits, lengths, decay_rate, head_gain, states):
    sequences, local_heads = states.shape[0], states.shape[1]
    heads = 2 if local_heads % 2 == 0 else 1
    groups = local_heads // heads
    local_rows = projected.shape[0]
    per_head = REFLECT + 1
    rates = rate_logits.reshape(local_rows, groups, heads * per_head).transpose(1, 0, 2)
    wide = heads * (2 * REFLECT + 1) * HEAD_DIM
    smem = pl.BlockSpec(memory_space=pltpu.SMEM)
    state_spec = pl.BlockSpec((1, heads, HEAD_DIM, HEAD_DIM), lambda s, g: (s, g, 0, 0))
    steps = pltpu.VMEM((heads, STEPS, HEAD_DIM), F32)
    return pl.pallas_call(
        functools.partial(mixer_kernel, heads),
        grid=(sequences, groups),
        in_specs=[
            smem,
            smem,
            pl.BlockSpec((NEW_POSITIONS, wide), lambda s, g: (s, g)),
            pl.BlockSpec((NEW_POSITIONS, 1), lambda s, g: (s, 0)),
            pl.BlockSpec((1, NEW_POSITIONS, heads * per_head), lambda s, g: (g, s, 0)),
            pl.BlockSpec((1, HEAD_DIM), lambda s, g: (0, 0)),
            state_spec,
        ],
        out_specs=[
            pl.BlockSpec((NEW_POSITIONS, heads * HEAD_DIM), lambda s, g: (s, g)),
            state_spec,
        ],
        out_shape=[
            jax.ShapeDtypeStruct((local_rows, local_heads * HEAD_DIM), BF16),
            jax.ShapeDtypeStruct(states.shape, F32),
        ],
        scratch_shapes=[steps, steps, steps],
        cost_estimate=pl.CostEstimate(
            flops=sequences * local_heads * 2 * 10**8, bytes_accessed=2**24, transcendentals=2**22
        ),
        name="mixer",
    )(lengths, decay_rate, projected, inverse, rates, head_gain[None], states)


def head_gather(own_ref, slots_ref, near_sem, far_send, far_recv, pass_send, pass_recv):
    chips = lax.axis_size("head") // 2
    me = lax.axis_index("head")
    chip, core = me // 2, lax.rem(me, 2)
    partner = 2 * chip + 1 - core

    def source(shift, flip):
        other = lax.rem(chip - shift + chips, chips)
        return 2 * other + (1 - core if flip else core)

    def near(r, slot):
        return pltpu.make_async_remote_copy(
            src_ref=own_ref.at[r],
            dst_ref=slots_ref.at[slot, r],
            send_sem=near_sem.at[0, r],
            recv_sem=near_sem.at[1, r],
            device_id={"head": partner},
            device_id_type=MESH,
        )

    def far(shift, r, slot):
        return pltpu.make_async_remote_copy(
            src_ref=own_ref.at[r],
            dst_ref=slots_ref.at[slot, r],
            send_sem=far_send.at[shift, r],
            recv_sem=far_recv.at[shift, r],
            device_id={"head": 2 * lax.rem(chip + shift, chips) + core},
            device_id_type=MESH,
        )

    def passed(shift, r, slot):
        return pltpu.make_async_remote_copy(
            src_ref=slots_ref.at[slot, r],
            dst_ref=slots_ref.at[slot, r],
            send_sem=pass_send.at[shift, r],
            recv_sem=pass_recv.at[shift, r],
            device_id={"head": partner},
            device_id_type=MESH,
        )

    def start():
        for r in range(PIECES):
            for shift in range(1, chips):
                far(shift, r, me).start()
        for r in range(PIECES):
            near(r, me).start()

    def wait_near():
        for r in range(PIECES):
            near(r, partner).wait_recv()

    def wait_far(r):
        for shift in range(1, chips):
            far(shift, r, source(shift, False)).wait_recv()
            passed(shift, r, source(shift, False)).start()
        for shift in range(1, chips):
            passed(shift, r, source(shift, True)).wait_recv()

    def drain():
        for r in range(PIECES):
            near(r, me).wait_send()
            for shift in range(1, chips):
                far(shift, r, me).wait_send()
                passed(shift, r, source(shift, False)).wait_send()

    order = [source(s, f) for s in range(chips) for f in (False, True)]
    return start, wait_near, wait_far, drain, order


def gather_scratch(head_count, rows, width):
    chips = max(head_count // 2, 1)
    pairs = pltpu.SemaphoreType.DMA((chips, PIECES))
    return [
        pltpu.VMEM((head_count, PIECES, rows // PIECES, width), BF16),
        pltpu.SemaphoreType.DMA((2, PIECES)),
        pairs,
        pairs,
        pairs,
        pairs,
    ]


def project_kernel(
    model_width,
    own_ref,
    gain_ref,
    rate_weight_ref,
    mix_hbm,
    proj_hbm,
    inverse_ref,
    rates_ref,
    mix_ref,
    scaled_ref,
    total_ref,
    mix_sem,
    out_sem,
    slots_ref,
    *gather_sems,
):
    head_count = lax.axis_size("head")
    me = lax.axis_index("head")
    start, wait_near, wait_far, drain, order = head_gather(own_ref, slots_ref, *gather_sems)
    half = own_ref.shape[1]
    rows = PIECES * half
    tile = mix_ref.shape[2] // (2 * REFLECT + 1)

    def load(slot):
        return pltpu.make_async_copy(mix_hbm.at[slot], mix_ref.at[slot], mix_sem.at[slot])

    for slot in order:
        load(slot).start()
    barrier = pltpu.get_barrier_semaphore()
    for k in range(1, head_count):
        pl.semaphore_signal(
            barrier, inc=1, device_id={"head": lax.rem(me + k, head_count)}, device_id_type=MESH
        )
    pl.semaphore_wait(barrier, head_count - 1)
    start()

    def prepare(ref, slot, r):
        wide = ref.astype(F32)
        scaled = (wide * gain_ref[slot]).astype(BF16)
        scaled_ref[slot, r * half : (r + 1) * half, :] = scaled
        square = jnp.sum(wide * wide, axis=1, keepdims=True)
        return square, jnp.dot(scaled, rate_weight_ref[slot], preferred_element_type=F32)

    squares, rates = [], []
    for r in range(PIECES):
        square, rate = prepare(own_ref[r], order[0], r)
        squares.append(square)
        rates.append(rate)
    load(order[0]).wait()

    @pl.loop(0, 2 * REFLECT + 1)
    def _(t):
        columns = pl.ds(pl.multiple_of(t * tile, HEAD_DIM), tile)
        total_ref[:, columns] = jnp.dot(
            scaled_ref[order[0]], mix_ref[order[0], :, columns], preferred_element_type=F32
        )

    wait_near()
    for r in range(PIECES):
        square, rate = prepare(slots_ref[order[1], r], order[1], r)
        squares[r], rates[r] = squares[r] + square, rates[r] + rate
    load(order[1]).wait()

    @pl.loop(0, 2 * REFLECT + 1)
    def _(t):
        columns = pl.ds(pl.multiple_of(t * tile, HEAD_DIM), tile)
        total_ref[:, columns] += jnp.dot(
            scaled_ref[order[1]], mix_ref[order[1], :, columns], preferred_element_type=F32
        )

    for slot in order[2:]:
        load(slot).wait()
    outs = []
    for r in range(PIECES):
        wait_far(r)
        here = slice(r * half, (r + 1) * half)
        for slot in order[2:]:
            square, rate = prepare(slots_ref[slot, r], slot, r)
            squares[r], rates[r] = squares[r] + square, rates[r] + rate
        inverse_ref[here, :] = lax.rsqrt(squares[r] / model_width + ROW_EPSILON)
        rates_ref[here, :] = rates[r]

        @pl.loop(0, 2 * REFLECT + 1)
        def _(t):
            columns = pl.ds(pl.multiple_of(t * tile, HEAD_DIM), tile)
            partial = total_ref[here, columns]
            for slot in order[2:]:
                partial = partial + jnp.dot(
                    scaled_ref[slot, here, :],
                    mix_ref[slot, :, columns],
                    preferred_element_type=F32,
                )
            total_ref[here, columns] = partial

        out = pltpu.make_async_copy(
            total_ref.at[pl.ds(r * half, half)], proj_hbm.at[pl.ds(r * half, half)], out_sem.at[r]
        )
        out.start()
        outs.append(out)
    drain()
    for out in outs:
        out.wait()


def project(tokens, norm_gain, mix_weight, rate_weight):
    head_count = lax.axis_size("head")
    rows, width = tokens.shape
    columns, rate_columns = mix_weight.shape[1], rate_weight.shape[1]
    vmem = pl.BlockSpec(memory_space=pltpu.VMEM)
    hbm = pl.BlockSpec(memory_space=pl.ANY)
    return pl.pallas_call(
        functools.partial(project_kernel, norm_gain.shape[0]),
        out_shape=[
            jax.ShapeDtypeStruct((rows, columns), F32),
            jax.ShapeDtypeStruct((rows, 1), F32),
            jax.ShapeDtypeStruct((rows, rate_columns), F32),
        ],
        in_specs=[vmem, vmem, vmem, hbm],
        out_specs=[hbm, vmem, vmem],
        scratch_shapes=[
            pltpu.VMEM((head_count, width, columns), BF16),
            pltpu.VMEM((head_count, rows, width), BF16),
            pltpu.VMEM((rows, columns), F32),
            pltpu.SemaphoreType.DMA((head_count,)),
            pltpu.SemaphoreType.DMA((PIECES,)),
        ]
        + gather_scratch(head_count, rows, width),
        compiler_params=pltpu.CompilerParams(collective_id=2, has_side_effects=True),
        name="project",
    )(
        tokens.reshape(PIECES, rows // PIECES, width),
        norm_gain.reshape(head_count, 1, width),
        rate_weight.reshape(head_count, width, rate_columns),
        mix_weight.reshape(head_count, width, columns),
    )


def swapped_weights(out_weight, width):
    head_count = lax.axis_size("head")
    chips = head_count // 2
    me = lax.axis_index("head")
    chip, core = me // 2, lax.rem(me, 2)
    pieces = []
    for shift in range(chips):
        for flip in range(2):
            to = 2 * lax.rem(chip + shift, chips) + lax.rem(core + flip, 2)
            piece = lax.dynamic_slice_in_dim(out_weight, to * width, width, axis=1)
            if shift or flip:
                route = [
                    (2 * a + b, 2 * ((a + shift) % chips) + (b + flip) % 2)
                    for a in range(chips)
                    for b in range(2)
                ]
                piece = lax.ppermute(piece, "head", route)
            pieces.append(piece)
    return pieces


def finish_kernel(batch_count, head_count, *refs):
    lengths_ref, own_ref, tokens_ref, gain_ref, next_ref, table_hbm = refs[:6]
    weights_hbm = refs[6 : 6 + head_count]
    (
        mixed_ref,
        out_ref,
        weight_ref,
        sum_ref,
        last_ref,
        table_ref,
        rows_ref,
        wide_ref,
        stat_ref,
        stats_ref,
        table_sem,
        weight_sem,
        row_send,
        row_recv,
        stat_send,
        stat_recv,
        slots_ref,
    ) = refs[6 + head_count : 23 + head_count]
    gather_sems = refs[23 + head_count :]
    count = batch_count * head_count
    batch_at, head_at = lax.axis_index("batch"), lax.axis_index("head")
    me = batch_at * head_count + head_at
    sequences, width = last_ref.shape
    half = own_ref.shape[1]
    vocab_here = table_ref.shape[0]
    start, wait_near, wait_far, drain, order = head_gather(own_ref, slots_ref, *gather_sems)

    loads = [
        pltpu.make_async_copy(weights_hbm[k], weight_ref.at[k], weight_sem.at[k])
        for k in range(head_count)
    ]
    for load in loads:
        load.start()
    table_load = pltpu.make_async_copy(table_hbm, table_ref, table_sem)
    table_load.start()

    def other(k):
        index = lax.rem(me + k, count)
        return index, {"batch": index // head_count, "head": lax.rem(index, head_count)}

    barrier = pltpu.get_barrier_semaphore()

    @pl.loop(1, count)
    def _(k):
        pl.semaphore_signal(barrier, inc=1, device_id=other(k)[1], device_id_type=MESH)

    pl.semaphore_wait(barrier, count - 1)
    start()
    for load in loads:
        load.wait()
    for r in range(PIECES):
        here = slice(r * half, (r + 1) * half)
        sum_ref[here, :] = jnp.dot(own_ref[r], weight_ref[0], preferred_element_type=F32)
    wait_near()
    for r in range(PIECES):
        here = slice(r * half, (r + 1) * half)
        sum_ref[here, :] += jnp.dot(
            slots_ref[order[1], r], weight_ref[1], preferred_element_type=F32
        )
    for r in range(PIECES):
        wait_far(r)
        here = slice(r * half, (r + 1) * half)
        partial = sum_ref[here, :]
        for k in range(2, head_count):
            partial = partial + jnp.dot(
                slots_ref[order[k], r], weight_ref[k], preferred_element_type=F32
            )
        sum_ref[here, :] = tokens_ref[here, :].astype(F32) + partial
    position = lax.broadcasted_iota(jnp.int32, (NEW_POSITIONS, width), 0)
    for s in range(sequences):
        here = slice(s * NEW_POSITIONS, (s + 1) * NEW_POSITIONS)
        block = sum_ref[here, :]
        chosen = jnp.where(position == lengths_ref[s] - 1, block, 0.0)
        last_ref[s : s + 1, :] = (
            jnp.sum(chosen, axis=0, keepdims=True).astype(BF16).astype(F32)
        )
    for r in range(PIECES):
        here = slice(r * half, (r + 1) * half)
        mixed_ref[here, :] = sum_ref[here, :].astype(BF16)

    def row_copy(k, slot):
        return pltpu.make_async_remote_copy(
            src_ref=last_ref,
            dst_ref=rows_ref.at[slot],
            send_sem=row_send.at[k],
            recv_sem=row_recv.at[slot],
            device_id=other(k)[1],
            device_id_type=MESH,
        )

    @pl.loop(1, count)
    def _(k):
        row_copy(k, me).start()

    rows_ref[me] = last_ref[...]
    drain()

    @pl.loop(1, count)
    def _(k):
        row_copy(k, other(k)[0]).wait_recv()

    for b in range(batch_count):
        for h in range(head_count):
            wide_ref[b * sequences : (b + 1) * sequences, h * width : (h + 1) * width] = rows_ref[
                b * head_count + h
            ]
    everyone = wide_ref[...]
    factor = lax.rsqrt(jnp.mean(everyone * everyone, axis=1, keepdims=True) + ROW_EPSILON)
    hidden = (everyone * factor * gain_ref[...]).astype(BF16)
    table_load.wait()
    logits = lax.dot_general(
        table_ref[...], hidden, (((1,), (1,)), ((), ())), preferred_element_type=F32
    )
    ids = lax.broadcasted_iota(jnp.int32, logits.shape, 0) + me * vocab_here
    largest = jnp.max(logits, axis=0, keepdims=True)
    stat_ref[0:1, :] = largest
    stat_ref[1:2, :] = jnp.sum(jnp.exp(logits - largest), axis=0, keepdims=True)
    stat_ref[2:3, :] = jnp.sum(
        jnp.where(ids == next_ref[...], logits, 0.0), axis=0, keepdims=True
    )
    stat_ref[3:, :] = jnp.zeros((stat_ref.shape[0] - 3, stat_ref.shape[1]), F32)

    def stat_copy(k, slot):
        return pltpu.make_async_remote_copy(
            src_ref=stat_ref,
            dst_ref=stats_ref.at[slot],
            send_sem=stat_send.at[k],
            recv_sem=stat_recv.at[slot],
            device_id=other(k)[1],
            device_id_type=MESH,
        )

    @pl.loop(1, count)
    def _(k):
        stat_copy(k, me).start()

    stats_ref[me] = stat_ref[...]

    @pl.loop(1, count)
    def _(k):
        row_copy(k, me).wait_send()
        stat_copy(k, other(k)[0]).wait_recv()

    highest = lax.fori_loop(
        0, count, lambda d, top: jnp.maximum(top, stats_ref[d][0:1]), largest
    )

    def add(d, totals):
        entry = stats_ref[d]
        return (totals[0] + entry[1:2] * jnp.exp(entry[0:1] - highest), totals[1] + entry[2:3])

    zero = jnp.zeros_like(largest)
    summed, target = lax.fori_loop(0, count, add, (zero, zero))
    out_ref[...] = target - (highest + jnp.log(summed))

    @pl.loop(1, count)
    def _(k):
        stat_copy(k, me).wait_send()


def finish(normed, weights, tokens, lengths, final_gain, vocab_table, next_token):
    batch_count, head_count = lax.axis_size("batch"), lax.axis_size("head")
    count = batch_count * head_count
    rows, width = tokens.shape
    sequences = lengths.shape[0]
    everyone = next_token.shape[0]
    vmem = pl.BlockSpec(memory_space=pltpu.VMEM)
    hbm = pl.BlockSpec(memory_space=pl.ANY)
    semaphores = pltpu.SemaphoreType.DMA((count,))
    mixed, scores = pl.pallas_call(
        functools.partial(finish_kernel, batch_count, head_count),
        out_shape=[
            jax.ShapeDtypeStruct((rows, width), BF16),
            jax.ShapeDtypeStruct((1, everyone), F32),
        ],
        in_specs=[pl.BlockSpec(memory_space=pltpu.SMEM), vmem, vmem, vmem, vmem, hbm]
        + [hbm] * head_count,
        out_specs=[vmem, vmem],
        scratch_shapes=[
            pltpu.VMEM((head_count,) + weights[0].shape, BF16),
            pltpu.VMEM((rows, width), F32),
            pltpu.VMEM((sequences, width), F32),
            pltpu.VMEM(vocab_table.shape, BF16),
            pltpu.VMEM((count, sequences, width), F32),
            pltpu.VMEM((everyone, final_gain.shape[0]), F32),
            pltpu.VMEM((8, everyone), F32),
            pltpu.VMEM((count, 8, everyone), F32),
            pltpu.SemaphoreType.DMA,
            pltpu.SemaphoreType.DMA((head_count,)),
            semaphores,
            semaphores,
            semaphores,
            semaphores,
        ]
        + gather_scratch(head_count, rows, normed.shape[1]),
        compiler_params=pltpu.CompilerParams(collective_id=1, has_side_effects=True),
        name="finish",
    )(
        lengths,
        normed.reshape(PIECES, rows // PIECES, normed.shape[1]),
        tokens,
        final_gain[None],
        next_token[None],
        vocab_table,
        *weights,
    )
    return mixed, scores[0]


def on_device(
    tokens,
    lengths,
    states,
    norm_gain,
    mix_weight,
    rate_weight,
    decay_rate,
    head_gain,
    out_weight,
    final_gain,
    vocab_table,
    next_token,
):
    projected, inverse, rate_logits = project(tokens, norm_gain, mix_weight, rate_weight)
    out_weight, inverse = lax.optimization_barrier((out_weight, inverse))
    weights = swapped_weights(out_weight, tokens.shape[1])
    normed, new_state = mixer(
        projected, inverse, rate_logits, lengths, decay_rate, head_gain, states
    )
    mixed, log_likelihood = finish(
        normed, weights, tokens, lengths, final_gain, vocab_table, next_token
    )
    return (mixed, new_state, log_likelihood)


def solution(mesh):
    placed = (
        P("batch", "head"),
        P("batch"),
        P("batch", "head", None, None),
        P(),
        P(None, "head"),
        P(None, "head"),
        P("head"),
        P(),
        P("head", None),
        P(),
        P(("batch", "head"), None),
        P(),
    )
    return jax.shard_map(
        on_device,
        mesh=mesh,
        in_specs=placed,
        out_specs=(P("batch", "head"), P("batch", "head", None, None), P()),
        check_vma=False,
    )
```
